32 devices in a mesh: pairs: 16 (over z, y, x), comp: 2 (over core).
Axes of the slice: x: 2, y: 2, z: 4, core: 2. Of those that a mesh axis runs over, the one named last changes fastest.
Arguments:
- effects: float32 [49, 131072], P(None, 'pairs'), may hold values from -24 to 24
- se_table: float32 [16, 49], replicated, may hold values from 0.5 to 2
- se_index: int32 [256], P('pairs'), may hold values from 0 to 15
- base_root: float32 [16, 49, 49], replicated, may hold values from -0.875 to 0.875
- grid_scale: float32 [16], replicated, may hold values from 0.25 to 4
- comp_base: int32 [256], P('comp'), may hold values from 0 to 15
- comp_grid: int32 [256], P('comp'), may hold values from 0 to 15
- weights: float32 [256], P('comp'), may hold values from 0.2 to 5
Outputs:
- responsibility: float32 [256, 131072], P('comp', 'pairs')
- log_weights: float32 [256], P('comp')
- pair_loglik: float32 [131072], P('pairs')
The draws below stay inside these ranges and needn't reach their ends.
All inputs are finite; a program needn't handle non-finite values.
Results may differ from the reference program's by a relative error of at most 0.0003.
Values sent between devices are 32-bit elements; how exact they have to be, the bound alone decides.
A program may use at most 384 MiB of HBM per device.

```python
import math
import jax
import jax.numpy as jnp
from jax import lax

R = 49
NU = 16
NGRID = 16
NB = 16
TILE = 512
PAIRS = 131072
K = 256


def draw_effects(key, part):
    key_scale, key_base, key_flag, key_sign = jax.random.split(key, 4)
    values = 1.5 * jax.random.normal(key_base, (R, PAIRS), dtype=jnp.float32)
    return jnp.clip(values, -8.0, 8.0).astype(jnp.float32)


def plant(entries, rng, low, top_value):
    longest = entries.shape.index(max(entries.shape))
    spots = []
    for shift in (0, 1):
        where = [jax.random.randint(jax.random.fold_in(rng, axis), (), 0, length) for axis, length in enumerate(entries.shape)]
        where[longest] = (where[longest] + shift) % entries.shape[longest]
        spots.append(tuple(where))
    return entries.at[spots[0]].set(low).at[spots[1]].set(top_value)


def steps_of(stream_key, extent, pieces, least, top_value):
    gain, own = 1.0, jax.random.fold_in(stream_key, 6)
    for axis_at, blocks in pieces:
        heights = jnp.exp(jax.random.uniform(jax.random.fold_in(own, axis_at), (blocks,), jnp.float32, least / len(pieces), top_value / len(pieces)))
        gain = gain * jnp.repeat(heights, extent[axis_at] // blocks).reshape([-1 if axis == axis_at else 1 for axis in range(len(extent))])
    return gain


def normal_values(stream_key, shape, deviation, most, kind=jnp.bfloat16):
    return jnp.clip(deviation * jax.random.normal(stream_key, shape, jnp.float32), -most, most).astype(kind)


def setup_inputs(seed: int = 0) -> dict:
    arg_keys = jax.random.split(jax.random.key(seed), 9)
    return {
        "effects": draw_effects(jax.random.fold_in(arg_keys[8], 71), 0),
        "se_table": jnp.clip(jnp.exp(jax.random.uniform(arg_keys[1], (NB, R), jnp.float32, math.log(0.5), math.log(2.0))), 0.5, 2.0),
        "se_index": plant(jax.random.randint(arg_keys[2], (PAIRS // TILE,), 0, NB), jax.random.fold_in(arg_keys[2], 1), 0, NB - 1).astype(jnp.int32),
        "base_root": normal_values(arg_keys[3], (NU, R, R), R ** -0.5, 0.875, jnp.float32),
        "grid_scale": jnp.clip(jnp.exp(jax.random.uniform(arg_keys[4], (NGRID,), jnp.float32, math.log(0.25), math.log(4.0))), 0.25, 4.0),
        "comp_base": plant(jax.random.randint(arg_keys[5], (K,), 0, NU), jax.random.fold_in(arg_keys[5], 1), 0, NU - 1).astype(jnp.int32),
        "comp_grid": plant(jax.random.randint(arg_keys[6], (K,), 0, NGRID), jax.random.fold_in(arg_keys[6], 1), 0, NGRID - 1).astype(jnp.int32),
        "weights": jnp.clip(jnp.exp(math.log(5.0) - 3.218876 * jax.random.uniform(arg_keys[7], (K,), jnp.float32) ** steps_of(arg_keys[7], (K,), ((0, 2),), -0.2, 0.2)), 0.2, 5.0),
    }


def whiten_tables(se_table, base_root, grid_scale, comp_base, comp_grid):
    covariances = jnp.einsum('uij,ukj->uik', base_root, base_root, precision=lax.Precision.HIGHEST)
    picked = covariances[comp_base]
    scales = grid_scale[comp_grid]
    identity = jnp.eye(R, dtype=base_root.dtype)
    system = (scales * scales)[None, :, None, None] * picked[None]
    system = system + identity[None, None] * (se_table * se_table)[:, None, :, None]
    factor = jnp.linalg.cholesky(system)
    eye_full = jnp.broadcast_to(identity, factor.shape)
    inverse = jax.scipy.linalg.solve_triangular(factor, eye_full, lower=True)
    half_logdet = jnp.sum(jnp.log(jnp.diagonal(factor, axis1=2, axis2=3)), axis=-1)
    return (inverse, half_logdet)

def reference(effects, se_table, se_index, base_root, grid_scale, comp_base, comp_grid, weights):
    inverse, half_logdet = whiten_tables(se_table, base_root, grid_scale, comp_base, comp_grid)
    log_prior = jnp.log(weights)
    constant = 0.5 * R * math.log(2.0 * math.pi)
    tile_rows = effects.reshape(R, PAIRS // TILE, TILE).transpose(1, 0, 2)

    def one_tile(inputs):
        block_id, tile_data = inputs
        whitened = jnp.einsum('kij,jp->kip', inverse[block_id], tile_data, precision=lax.Precision.HIGHEST)
        quadratic = jnp.sum(whitened * whitened, axis=1)
        return log_prior[:, None] - 0.5 * quadratic - half_logdet[block_id][:, None] - constant
    scores = lax.map(one_tile, (se_index.astype(jnp.int32), tile_rows))
    scores = scores.transpose(1, 0, 2).reshape(K, PAIRS)
    score_max = jnp.max(scores, axis=0)
    score_sum = jnp.sum(jnp.exp(scores - score_max), axis=0)
    pair_loglik = score_max + jnp.log(score_sum)
    responsibility = jnp.exp(scores - pair_loglik)
    masses = jnp.sum(responsibility, axis=1)
    log_weights = jnp.log((masses + 1.0) / (PAIRS + K))
    return (responsibility, log_weights, pair_loglik)
```

```python
import math

import jax
import jax.numpy as jnp
from jax import lax
from jax.experimental import pallas as pl
from jax.experimental.pallas import tpu as pltpu
from jax.sharding import PartitionSpec as P

SUB = 8


def exact_dot(left, right):
    return jnp.dot(left, right, precision=lax.Precision.HIGHEST, preferred_element_type=jnp.float32)


def split_terms(value):
    high = value.astype(jnp.bfloat16)
    return high, (value - high.astype(jnp.float32)).astype(jnp.bfloat16)


def factor_pattern(pattern, se_square, covar, upper, inverse, table, prior, bias, tissues, constant):
    blocks = -(-tissues // SUB)
    comps = covar.shape[2]
    slot = table.shape[1] // 4
    sub_iota = lax.broadcasted_iota(jnp.int32, (SUB, comps), 0)
    half_logdet = jnp.zeros((1, comps), jnp.float32)
    for first in range(0, tissues, 4):
        row_block = first // SUB
        rows = range(first, min(first + 4, tissues))
        system, solved = {}, {}
        for row in rows:
            system[row] = [covar[row, v * SUB : (v + 1) * SUB, :] for v in range(row_block, blocks)]
            on_diag = sub_iota == row % SUB
            system[row][0] = system[row][0] + jnp.where(on_diag, se_square[pattern, row], 0.0)
            solved[row] = [jnp.zeros((SUB, comps), jnp.float32) for _ in range(row_block)]
            solved[row].append(jnp.where(on_diag, 1.0, 0.0))
        for col in range(first):
            col_block = col // SUB
            up = [upper[col, v * SUB : (v + 1) * SUB, :] for v in range(row_block, blocks)]
            inv = [inverse[col, v * SUB : (v + 1) * SUB, :] for v in range(col_block + 1)]
            for row in rows:
                mult = upper[col, row : row + 1, :]
                for n, part in enumerate(up):
                    system[row][n] = system[row][n] - mult * part
                for n, part in enumerate(inv):
                    solved[row][n] = solved[row][n] - mult * part
        for row in rows:
            pivot = system[row][0][row % SUB : row % SUB + 1, :]
            root = lax.rsqrt(pivot)
            root = root * (1.5 - 0.5 * pivot * root * root)
            half_logdet = half_logdet + 0.5 * jnp.log(pivot)
            up = [part * root for part in system[row]]
            inv = [part * root for part in solved[row]]
            for n, part in enumerate(up):
                upper[row, (row_block + n) * SUB : (row_block + n + 1) * SUB, :] = part
            for n, part in enumerate(inv):
                inverse[row, n * SUB : (n + 1) * SUB, :] = part
            for later in rows:
                if later > row:
                    mult = up[0][later % SUB : later % SUB + 1, :]
                    for n, part in enumerate(up):
                        system[later][n] = system[later][n] - mult * part
                    for n, part in enumerate(inv):
                        solved[later][n] = solved[later][n] - mult * part
            if len(inv) % 2:
                inv = inv + [jnp.zeros((SUB, comps), jnp.float32)]
            high, low = split_terms(jnp.concatenate(inv, axis=0))
            lanes = slice((row % 2) * comps, (row % 2 + 1) * comps)
            height = len(inv) * SUB
            table[row // 2, 0:height, lanes] = high
            table[row // 2, slot : slot + height, lanes] = high
            table[row // 2, 2 * slot : 2 * slot + height, lanes] = low
            table[row // 2, 3 * slot : 3 * slot + height, lanes] = low
    bias[...] = jnp.log(prior[...]) - half_logdet - constant


def make_body(tissues):
    constant = 0.5 * tissues * math.log(2.0 * math.pi)

    def body(order, patterns, se_square, effects, covar, prior, scores, peak, total,
             upper, inverse, table, bias, quad, wide):
        step = pl.program_id(0)
        slot = table.shape[1] // 4
        comps = covar.shape[2]

        @pl.when(step == 0)
        def _():
            table[...] = jnp.zeros(table.shape, table.dtype)
            wide[...] = jnp.zeros(wide.shape, wide.dtype)

        fresh = jnp.logical_or(
            step == 0, patterns[step] != patterns[jnp.maximum(step - 1, 0)]
        )

        @pl.when(fresh)
        def _():
            factor_pattern(patterns[step], se_square, covar, upper, inverse, table, prior, bias,
                           tissues, constant)

        tile = effects[...]
        high = tile.astype(jnp.bfloat16).astype(jnp.float32)
        wide[0:tissues, :] = high
        wide[slot : slot + tissues, :] = tile - high
        turned = wide[...].T.astype(jnp.bfloat16)
        packed = jnp.concatenate([turned, turned], axis=1)
        quad[...] = jnp.zeros(quad.shape, quad.dtype)

        def pair_of_rows(index, carry):
            white = jnp.dot(packed, table[index], preferred_element_type=jnp.float32)
            white = white * white
            quad[...] += white[:, :comps] + white[:, comps:]
            return carry

        lax.fori_loop(0, table.shape[0], pair_of_rows, 0)
        found = (bias[...] - 0.5 * quad[...]).T
        scores[...] = found
        top = jnp.max(found, axis=0, keepdims=True)
        peak[...] = top
        total[...] = jnp.sum(jnp.exp(found - top), axis=0, keepdims=True)

    return body


def score_tiles(effects, se_table, se_index, covar, weights):
    tissues, pairs = effects.shape
    tiles = se_index.shape[0]
    comps = weights.shape[0]
    width = pairs // tiles
    padded = covar.shape[1]
    slot = 16 * (-(-tissues // 16))
    place = jnp.arange(tiles, dtype=jnp.int32)
    before = (se_index[None, :] < se_index[:, None]) | (
        (se_index[None, :] == se_index[:, None]) & (place[None, :] < place[:, None])
    )
    rank = jnp.sum(before.astype(jnp.int32), axis=1)
    hit = rank[None, :] == place[:, None]
    order = jnp.sum(jnp.where(hit, place[None, :], 0), axis=1)
    patterns = jnp.sum(jnp.where(hit, se_index[None, :], 0), axis=1)
    grid_spec = pltpu.PrefetchScalarGridSpec(
        num_scalar_prefetch=3,
        grid=(tiles,),
        in_specs=[
            pl.BlockSpec((tissues, width), lambda t, order, *_: (0, order[t])),
            pl.BlockSpec(covar.shape, lambda t, *_: (0, 0, 0)),
            pl.BlockSpec((1, comps), lambda t, *_: (0, 0)),
        ],
        out_specs=[
            pl.BlockSpec((comps, width), lambda t, order, *_: (0, order[t])),
            pl.BlockSpec((1, width), lambda t, order, *_: (0, order[t])),
            pl.BlockSpec((1, width), lambda t, order, *_: (0, order[t])),
        ],
        scratch_shapes=[
            pltpu.VMEM((tissues, padded, comps), jnp.float32),
            pltpu.VMEM((tissues, padded, comps), jnp.float32),
            pltpu.VMEM(((tissues + 1) // 2, 4 * slot, 2 * comps), jnp.bfloat16),
            pltpu.VMEM((1, comps), jnp.float32),
            pltpu.VMEM((width, comps), jnp.float32),
            pltpu.VMEM((2 * slot, width), jnp.float32),
        ],
    )
    return pl.pallas_call(
        make_body(tissues),
        grid_spec=grid_spec,
        out_shape=[
            jax.ShapeDtypeStruct((comps, pairs), jnp.float32),
            jax.ShapeDtypeStruct((1, pairs), jnp.float32),
            jax.ShapeDtypeStruct((1, pairs), jnp.float32),
        ],
        compiler_params=pltpu.CompilerParams(
            dimension_semantics=("arbitrary",), vmem_limit_bytes=48 * 1024 * 1024
        ),
        name="score_tiles",
    )(order, patterns, se_table * se_table, effects, covar, weights[None])


def per_device(effects, se_table, se_index, base_root, grid_scale, comp_base, comp_grid, weights):
    tissues = effects.shape[0]
    comps = comp_base.shape[0]
    padded = SUB * (-(-tissues // SUB))
    right = jnp.pad(base_root, ((0, 0), (0, padded - tissues), (0, 0)))
    covariances = jnp.einsum("uij,ukj->uik", base_root, right, precision=lax.Precision.HIGHEST)
    base_pick = (
        jnp.arange(covariances.shape[0], dtype=jnp.int32)[:, None] == comp_base[None]
    ).astype(jnp.float32)
    grid_pick = (
        comp_grid[:, None] == jnp.arange(grid_scale.shape[0], dtype=jnp.int32)[None]
    )
    comp_scale = jnp.sum(jnp.where(grid_pick, grid_scale[None], 0.0), axis=1)
    covar = lax.dot_general(
        covariances.reshape(covariances.shape[0], tissues * padded),
        base_pick,
        (((0,), (0,)), ((), ())),
        precision=lax.Precision.HIGHEST,
        preferred_element_type=jnp.float32,
    )
    covar = (covar * (comp_scale * comp_scale)[None]).reshape(tissues, padded, comps)
    scores, peak, total = score_tiles(effects, se_table, se_index, covar, weights)
    part = jnp.concatenate([peak, total], axis=0)
    every = lax.all_gather(part, "comp")
    score_max = jnp.max(every[:, 0], axis=0)
    score_sum = jnp.sum(every[:, 1] * jnp.exp(every[:, 0] - score_max[None]), axis=0)
    pair_loglik = score_max + jnp.log(score_sum)
    responsibility = jnp.exp(scores - pair_loglik)
    masses = lax.psum(jnp.sum(responsibility, axis=1), "pairs")
    all_pairs = effects.shape[1] * lax.axis_size("pairs")
    all_comps = comps * lax.axis_size("comp")
    log_weights = jnp.log((masses + 1.0) / (all_pairs + all_comps))
    return (responsibility, log_weights, pair_loglik)


def solution(mesh):
    placed = (P(None, "pairs"), P(), P("pairs"), P(), P(), P("comp"), P("comp"), P("comp"))
    return jax.shard_map(
        per_device,
        mesh=mesh,
        in_specs=placed,
        out_specs=(P("comp", "pairs"), P("comp"), P("pairs")),
        check_vma=False,
    )
```

```python
import math

import jax
import jax.numpy as jnp
from jax import lax
from jax.experimental import pallas as pl
from jax.experimental.pallas import tpu as pltpu
from jax.sharding import PartitionSpec as P

SUB = 8


def exact_dot(left, right):
    return jnp.dot(left, right, precision=lax.Precision.HIGHEST, preferred_element_type=jnp.float32)


def split_terms(value):
    high = value.astype(jnp.bfloat16)
    return high, (value - high.astype(jnp.float32)).astype(jnp.bfloat16)


def factor_pattern(pattern, se_square, covar, upper, inverse, table, prior, bias, tissues, constant):
    blocks = -(-tissues // SUB)
    comps = covar.shape[2]
    slot = table.shape[1] // 4
    sub_iota = lax.broadcasted_iota(jnp.int32, (SUB, comps), 0)
    half_logdet = jnp.zeros((1, comps), jnp.float32)
    for first in range(0, tissues, 4):
        row_block = first // SUB
        rows = range(first, min(first + 4, tissues))
        system, solved = {}, {}
        for row in rows:
            system[row] = [covar[row, v * SUB : (v + 1) * SUB, :] for v in range(row_block, blocks)]
            on_diag = sub_iota == row % SUB
            system[row][0] = system[row][0] + jnp.where(on_diag, se_square[pattern, row], 0.0)
            solved[row] = [jnp.zeros((SUB, comps), jnp.float32) for _ in range(row_block)]
            solved[row].append(jnp.where(on_diag, 1.0, 0.0))
        for col in range(first):
            col_block = col // SUB
            up = [upper[col, v * SUB : (v + 1) * SUB, :] for v in range(row_block, blocks)]
            inv = [inverse[col, v * SUB : (v + 1) * SUB, :] for v in range(col_block + 1)]
            for row in rows:
                mult = upper[col, row : row + 1, :]
                for n, part in enumerate(up):
                    system[row][n] = system[row][n] - mult * part
                for n, part in enumerate(inv):
                    solved[row][n] = solved[row][n] - mult * part
        for row in rows:
            pivot = system[row][0][row % SUB : row % SUB + 1, :]
            root = lax.rsqrt(pivot)
            root = root * (1.5 - 0.5 * pivot * root * root)
            half_logdet = half_logdet + 0.5 * jnp.log(pivot)
            up = [part * root for part in system[row]]
            inv = [part * root for part in solved[row]]
            for n, part in enumerate(up):
                upper[row, (row_block + n) * SUB : (row_block + n + 1) * SUB, :] = part
            for n, part in enumerate(inv):
                inverse[row, n * SUB : (n + 1) * SUB, :] = part
            for later in rows:
                if later > row:
                    mult = up[0][later % SUB : later % SUB + 1, :]
                    for n, part in enumerate(up):
                        system[later][n] = system[later][n] - mult * part
                    for n, part in enumerate(inv):
                        solved[later][n] = solved[later][n] - mult * part
            if len(inv) % 2:
                inv = inv + [jnp.zeros((SUB, comps), jnp.float32)]
            high, low = split_terms(jnp.concatenate(inv, axis=0))
            lanes = slice((row % 2) * comps, (row % 2 + 1) * comps)
            height = len(inv) * SUB
            table[row // 2, 0:height, lanes] = high
            table[row // 2, slot : slot + height, lanes] = high
            table[row // 2, 2 * slot : 2 * slot + height, lanes] = low
            table[row // 2, 3 * slot : 3 * slot + height, lanes] = low
    bias[...] = jnp.log(prior[...]) - half_logdet - constant


def make_body(tissues):
    constant = 0.5 * tissues * math.log(2.0 * math.pi)

    def body(order, patterns, se_square, effects, covar, prior, scores, peak, total,
             upper, inverse, table, bias, quad, wide):
        step = pl.program_id(0)
        slot = table.shape[1] // 4
        comps = covar.shape[2]

        @pl.when(step == 0)
        def _():
            table[...] = jnp.zeros(table.shape, table.dtype)
            wide[...] = jnp.zeros(wide.shape, wide.dtype)

        fresh = jnp.logical_or(
            step == 0, patterns[step] != patterns[jnp.maximum(step - 1, 0)]
        )

        @pl.when(fresh)
        def _():
            factor_pattern(patterns[step], se_square, covar, upper, inverse, table, prior, bias,
                           tissues, constant)

        tile = effects[...]
        high = tile.astype(jnp.bfloat16).astype(jnp.float32)
        wide[0:tissues, :] = high
        wide[slot : slot + tissues, :] = tile - high
        turned = wide[...].T.astype(jnp.bfloat16)
        packed = jnp.concatenate([turned, turned], axis=1)
        for index in range(table.shape[0]):
            white = jnp.dot(packed, table[index], preferred_element_type=jnp.float32)
            white = white * white
            part = white[:, :comps] + white[:, comps:]
            if index == 0:
                quad[...] = part
            else:
                quad[...] += part
        found = (bias[...] - 0.5 * quad[...]).T
        scores[...] = found
        top = jnp.max(found, axis=0, keepdims=True)
        peak[...] = top
        total[...] = jnp.sum(jnp.exp(found - top), axis=0, keepdims=True)

    return body


def score_tiles(effects, se_table, se_index, covar, weights):
    tissues, pairs = effects.shape
    tiles = se_index.shape[0]
    comps = weights.shape[0]
    width = pairs // tiles
    padded = covar.shape[1]
    slot = 16 * (-(-tissues // 16))
    place = jnp.arange(tiles, dtype=jnp.int32)
    before = (se_index[None, :] < se_index[:, None]) | (
        (se_index[None, :] == se_index[:, None]) & (place[None, :] < place[:, None])
    )
    rank = jnp.sum(before.astype(jnp.int32), axis=1)
    hit = rank[None, :] == place[:, None]
    order = jnp.sum(jnp.where(hit, place[None, :], 0), axis=1)
    patterns = jnp.sum(jnp.where(hit, se_index[None, :], 0), axis=1)
    grid_spec = pltpu.PrefetchScalarGridSpec(
        num_scalar_prefetch=3,
        grid=(tiles,),
        in_specs=[
            pl.BlockSpec((tissues, width), lambda t, order, *_: (0, order[t])),
            pl.BlockSpec(covar.shape, lambda t, *_: (0, 0, 0)),
            pl.BlockSpec((1, comps), lambda t, *_: (0, 0)),
        ],
        out_specs=[
            pl.BlockSpec((comps, width), lambda t, order, *_: (0, order[t])),
            pl.BlockSpec((1, width), lambda t, order, *_: (0, order[t])),
            pl.BlockSpec((1, width), lambda t, order, *_: (0, order[t])),
        ],
        scratch_shapes=[
            pltpu.VMEM((tissues, padded, comps), jnp.float32),
            pltpu.VMEM((tissues, padded, comps), jnp.float32),
            pltpu.VMEM(((tissues + 1) // 2, 4 * slot, 2 * comps), jnp.bfloat16),
            pltpu.VMEM((1, comps), jnp.float32),
            pltpu.VMEM((width, comps), jnp.float32),
            pltpu.VMEM((2 * slot, width), jnp.float32),
        ],
    )
    return pl.pallas_call(
        make_body(tissues),
        grid_spec=grid_spec,
        out_shape=[
            jax.ShapeDtypeStruct((comps, pairs), jnp.float32),
            jax.ShapeDtypeStruct((1, pairs), jnp.float32),
            jax.ShapeDtypeStruct((1, pairs), jnp.float32),
        ],
        compiler_params=pltpu.CompilerParams(
            dimension_semantics=("arbitrary",), vmem_limit_bytes=48 * 1024 * 1024
        ),
        name="score_tiles",
    )(order, patterns, se_table * se_table, effects, covar, weights[None])


def per_device(effects, se_table, se_index, base_root, grid_scale, comp_base, comp_grid, weights):
    tissues = effects.shape[0]
    comps = comp_base.shape[0]
    padded = SUB * (-(-tissues // SUB))
    right = jnp.pad(base_root, ((0, 0), (0, padded - tissues), (0, 0)))
    covariances = jnp.einsum("uij,ukj->uik", base_root, right, precision=lax.Precision.HIGHEST)
    base_pick = (
        jnp.arange(covariances.shape[0], dtype=jnp.int32)[:, None] == comp_base[None]
    ).astype(jnp.float32)
    grid_pick = (
        comp_grid[:, None] == jnp.arange(grid_scale.shape[0], dtype=jnp.int32)[None]
    )
    comp_scale = jnp.sum(jnp.where(grid_pick, grid_scale[None], 0.0), axis=1)
    covar = lax.dot_general(
        covariances.reshape(covariances.shape[0], tissues * padded),
        base_pick,
        (((0,), (0,)), ((), ())),
        precision=lax.Precision.HIGHEST,
        preferred_element_type=jnp.float32,
    )
    covar = (covar * (comp_scale * comp_scale)[None]).reshape(tissues, padded, comps)
    scores, peak, total = score_tiles(effects, se_table, se_index, covar, weights)
    part = jnp.concatenate([peak, total], axis=0)
    every = lax.all_gather(part, "comp")
    score_max = jnp.max(every[:, 0], axis=0)
    score_sum = jnp.sum(every[:, 1] * jnp.exp(every[:, 0] - score_max[None]), axis=0)
    pair_loglik = score_max + jnp.log(score_sum)
    responsibility = jnp.exp(scores - pair_loglik)
    own_mass = jnp.sum(responsibility, axis=1)
    copies = jnp.broadcast_to(own_mass[None], (lax.axis_size("pairs"), comps))
    masses = jnp.sum(lax.all_to_all(copies, "pairs", 0, 0, tiled=True), axis=0)
    all_pairs = effects.shape[1] * lax.axis_size("pairs")
    all_comps = comps * lax.axis_size("comp")
    log_weights = jnp.log((masses + 1.0) / (all_pairs + all_comps))
    return (responsibility, log_weights, pair_loglik)


def solution(mesh):
    placed = (P(None, "pairs"), P(), P("pairs"), P(), P(), P("comp"), P("comp"), P("comp"))
    return jax.shard_map(
        per_device,
        mesh=mesh,
        in_specs=placed,
        out_specs=(P("comp", "pairs"), P("comp"), P("pairs")),
        check_vma=False,
    )
```
